32 devices in a mesh: sess: 16 (over z, x, core), exp: 2 (over y).
Axes of the slice: x: 2, y: 2, z: 4, core: 2. Of those that a mesh axis runs over, the one named last changes fastest.
Arguments:
- tokens: bfloat16 [16, 64, 4096], P('sess'), may hold values from -6 to 6
- routes: int32 [16, 64, 2], P('sess'), may hold values from 0 to 15, all different within a row; in each aligned block of 64 rows (0 to 63, 64 to 127, ..., all dimensions but the last counted through in order) at most 16 rows name the same one
- gates: float32 [16, 64, 2], P('sess'), may hold values from 0.2 to 1
- w_gate: bfloat16 [16, 4096, 1408], P('sess', None, 'exp'), may hold values from -0.09375 to 0.09375
- w_up: bfloat16 [16, 4096, 1408], P('sess', None, 'exp'), may hold values from -0.09375 to 0.09375
- w_down: bfloat16 [16, 1408, 4096], P('sess', 'exp'), may hold values from -0.15625 to 0.15625
- feat_gain: float32 [4096], replicated, may hold values from 0.25 to 1.75
- w_proj: bfloat16 [4096, 256], replicated, may hold values from -0.09375 to 0.09375
- conv_time: bfloat16 [3, 3, 3, 256, 256], replicated, may hold values from -0.078125 to 0.078125
- bias_time: float32 [256], replicated, may hold values from -3 to 3
- conv_space: bfloat16 [3, 3, 256, 256], replicated, may hold values from -0.125 to 0.125
- bias_space: float32 [256], replicated, may hold values from -3 to 3
- frame_cache: bfloat16 [3, 16, 16, 16, 256], P(None, 'sess', 'exp'), may hold values from -6 to 6
- cache_head: int32 [16], P('sess'), may hold values from 0 to 2
Outputs:
- out_frame: bfloat16 [16, 16, 16, 256], P('sess', 'exp')
The draws below stay inside these ranges and needn't reach their ends.
Inputs may be any that keep to these rules, and one draw needn't show every extreme that they name: `routes`: each token names 2 different experts; among the tokens of one session no expert is named more than 16 times, and in some sessions one is named exactly 16 times. The frame before the previous one is in slot (cache_head + 2) mod 3.
All inputs are finite; a program needn't handle non-finite values.
Results may differ from the reference program's by a relative error of at most 0.017.
Values may be sent and summed in bfloat16 or wider, within the bound.
A program may use at most 64 MiB of HBM per device.

```python
import math
import jax
import jax.numpy as jnp
import numpy as np
from jax import lax

D = 4096
HID = 1408
C = 256
TOPK = 2
GRID_W = 8
EXPERTS = 16
SESS = 16
GRID_H = 8
TOK_SESS = 64
CAP = 16
PH = 16
PW = 16
N_EXP = 2


def set_ends(drawn, key, low, largest):
    extent = drawn.shape
    place = [jax.random.randint(jax.random.fold_in(key, axis), (), 0, extent[axis]) for axis in range(len(extent))]
    drawn = drawn.at[tuple(place)].set(low)
    longest = extent.index(max(extent))
    place[longest] = (place[longest] + 1) % extent[longest]
    return drawn.at[tuple(place)].set(largest)


def block_levels(rng, extent, cuts, smallest, top_value):
    gain, own = 1.0, jax.random.fold_in(rng, 6)
    for dim, shards_of in cuts:
        draws = jnp.exp(jax.random.uniform(jax.random.fold_in(own, dim), (shards_of,), jnp.float32, smallest / len(cuts), top_value / len(cuts)))
        gain = gain * jnp.repeat(draws, extent[dim] // shards_of).reshape([-1 if axis == dim else 1 for axis in range(len(extent))])
    return gain


def shared_out(rng, own, number, rows, number_of, top, reach, slope):
    ranking = jax.random.permutation(rng, number_of)
    crowded, usual = portions_of(number_of, rows * top, reach, slope, True), portions_of(number_of, rows * top, reach, slope, False)
    places = jnp.arange(number_of)

    def named(lengths, turn):
        used = int((lengths > 0).sum())
        fixed = max(1, used // 4)
        shifted = fixed + (places - fixed + turn * (used - fixed)) % max(1, number_of - fixed)
        return jnp.zeros((number_of,), jnp.int32).at[ranking[jnp.where(places < fixed, places, shifted)]].set(jnp.asarray(lengths, jnp.int32))

    lengths = jnp.where(number % 4 == 0, named(crowded, number // 4), named(usual, number - number // 4 - 1))
    mixed = jax.random.permutation(jax.random.fold_in(own, 3), number_of)
    giver, sink = mixed[0:number_of // 2 * 2:2], mixed[1:number_of // 2 * 2:2]
    slack = jnp.minimum(lengths[giver] - 1, reach - lengths[sink]) // 2
    slack = jnp.where((giver == ranking[0]) | (sink == ranking[0]) | (lengths[sink] == 0), 0, jnp.maximum(slack, 0))
    shifted = jax.random.randint(jax.random.fold_in(own, 4), (number_of // 2,), 0, 1 << 20) % (slack + 1)
    lengths = lengths.at[giver].add(-shifted).at[sink].add(shifted)
    members = jnp.searchsorted(jnp.cumsum(lengths), jnp.arange(rows * top), side="right").astype(jnp.int32)
    table = members.reshape(top, rows).T
    table = table[jax.random.permutation(jax.random.fold_in(own, 1), rows)]
    turn = jax.random.randint(jax.random.fold_in(own, 2), (rows, 1), 0, top)
    return jnp.take_along_axis(table, (jnp.arange(top)[None, :] + turn) % top, axis=1)


def portions_of(number_of, total, limit, lean, full):
    weights = [(1 << 20) // math.isqrt(rank ** lean) + 1 for rank in range(1, number_of + 1)]
    largest = limit if full else min(limit, max(-(-total // number_of), total * weights[0] // sum(weights)))
    least = 1 if total - largest >= number_of - 1 else 0
    counts, spare = [largest] + [least] * (number_of - 1), total - largest - least * (number_of - 1)
    while spare > 0:
        movable = [i for i in range(1, number_of) if counts[i] < largest] or [i for i in range(1, number_of) if counts[i] < limit]
        whole, budget = sum([weights[i] for i in movable]), spare
        for i in movable:
            addition = min(limit - counts[i], max(1, budget * weights[i] // whole), spare)
            counts[i] = counts[i] + addition
            spare = spare - addition
    return np.array(counts)


def centred(rng, extent, scale, limit, cuts=(), kind=jnp.bfloat16):
    values = jax.random.normal(rng, extent, jnp.float32) * scale
    if len(cuts) > 0:
        values = block_levels(rng, extent, cuts, -0.22, 0.18) * values
    return jnp.clip(values, min=-limit, max=limit).astype(kind)


def setup_inputs(seed: int = 0) -> dict:
    keys = jax.random.split(jax.random.key(seed), 15)
    tokens = centred(keys[0], (SESS, TOK_SESS, D), 1.0, 6.0, ((0, 16),))
    routes_keys = jax.random.split(jax.random.fold_in(keys[1], 1), SESS * TOK_SESS // TOK_SESS)
    routes_turns = jax.random.permutation(jax.random.fold_in(keys[1], 3), SESS * TOK_SESS // TOK_SESS)
    routes = jax.vmap(lambda own, number: shared_out(jax.random.fold_in(keys[1], 2), own, number, TOK_SESS, EXPERTS, TOPK, CAP, 2))(routes_keys, routes_turns).reshape((SESS, TOK_SESS, TOPK))
    gates = jnp.clip(0.2 + 0.8 * jax.random.uniform(keys[2], (SESS, TOK_SESS, TOPK), jnp.float32) ** block_levels(keys[2], (SESS, TOK_SESS, TOPK), ((0, 16),), -0.2, 0.2), 0.2, 1.0)
    w_gate = centred(keys[3], (EXPERTS, D, HID), D ** -0.5, 0.09375, ((0, 16), (2, 2)))
    w_up = centred(keys[4], (EXPERTS, D, HID), D ** -0.5, 0.09375, ((0, 16), (2, 2)))
    w_down = centred(keys[5], (EXPERTS, HID, D), HID ** -0.5, 0.15625, ((0, 16), (1, 2)))
    feat_gain = jnp.clip(1.0 + 0.15 * jax.random.normal(keys[6], (D,), jnp.float32), 0.25, 1.75)
    w_proj = centred(keys[7], (D, C), D ** -0.5, 0.09375)
    conv_time = centred(keys[8], (3, 3, 3, C, C), (27 * C) ** -0.5, 0.078125)
    bias_time = centred(keys[9], (C,), 0.5, 3.0, (), jnp.float32)
    conv_space = centred(keys[10], (3, 3, C, C), (9 * C) ** -0.5, 0.125)
    bias_space = centred(keys[11], (C,), 0.5, 3.0, (), jnp.float32)
    frame_cache = centred(keys[12], (3, SESS, PH, PW, C), 1.0, 6.0, ((1, 16), (2, 2)))
    cache_head = set_ends(jax.random.randint(keys[13], (SESS,), 0, 3), jax.random.fold_in(keys[13], 1), 0, 2).astype(jnp.int32)
    return {"tokens": tokens, "routes": routes, "gates": gates, "w_gate": w_gate, "w_up": w_up, "w_down": w_down, "feat_gain": feat_gain, "w_proj": w_proj, "conv_time": conv_time, "bias_time": bias_time, "conv_space": conv_space, "bias_space": bias_space, "frame_cache": frame_cache, "cache_head": cache_head}


epsilon = 1e-06

def slot_targets(routes, experts, capacity):
    flat = routes.reshape(-1).astype(jnp.int32)
    onehot = (flat[:, None] == jnp.arange(experts, dtype=jnp.int32)[None, :]).astype(jnp.int32)
    before = jnp.cumsum(onehot, axis=0) - onehot
    position = lax.optimization_barrier(jnp.sum(before * onehot, axis=1))
    return (flat * capacity + position).astype(jnp.int32)

def pick_slot(cache, heads):
    choose = (jnp.arange(3, dtype=jnp.int32)[:, None] == heads[None, :]).astype(jnp.float32)
    return lax.optimization_barrier(jnp.sum(choose[:, :, None, None, None] * cache.astype(jnp.float32), axis=0)).astype(jnp.bfloat16)

def reference(tokens, routes, gates, w_gate, w_up, w_down, feat_gain, w_proj, conv_time, bias_time, conv_space, bias_space, frame_cache, cache_head):
    capacity = CAP
    slots = EXPERTS * capacity
    count = TOK_SESS * TOPK
    slice_width = HID // N_EXP
    dest = jax.vmap(lambda single: slot_targets(single, EXPERTS, capacity))(routes)
    filler = jnp.full((SESS, slots), count, jnp.int32)
    owner = jax.vmap(lambda base, target: base.at[target].set(jnp.arange(count, dtype=jnp.int32)))(filler, dest)
    padded = jnp.concatenate([tokens, jnp.zeros((SESS, 1, D), tokens.dtype)], axis=1)
    weights = jnp.concatenate([gates.reshape(SESS, count), jnp.zeros((SESS, 1), jnp.float32)], axis=1)
    session_ids = jnp.arange(SESS, dtype=jnp.int32)[:, None]

    def one_expert(total, expert):
        route_ids = lax.dynamic_slice_in_dim(owner, (expert * capacity).astype(jnp.int32), capacity, 1)
        token_ids = jnp.where(route_ids < count, route_ids // TOPK, TOK_SESS).astype(jnp.int32)
        rows = padded[session_ids, token_ids].reshape(SESS * capacity, D)
        gate = jnp.dot(rows, w_gate[expert], preferred_element_type=jnp.float32)
        upward = jnp.dot(rows, w_up[expert], preferred_element_type=jnp.float32)
        hidden = (jax.nn.silu(gate) * upward).astype(jnp.bfloat16)
        pieces = hidden.astype(jnp.float32).reshape(-1, N_EXP, slice_width)
        lowered = w_down[expert].astype(jnp.float32).reshape(N_EXP, slice_width, D)
        parts = jnp.einsum('rjh,jhd->rjd', pieces, lowered).astype(jnp.bfloat16)
        summed = lax.optimization_barrier(jnp.sum(parts.astype(jnp.float32), axis=1)).reshape(SESS, capacity, D)
        scale = weights[session_ids, route_ids]
        total = total.at[session_ids, token_ids].add(scale[:, :, None] * summed)
        return (total, None)
    start_total = jnp.zeros((SESS, TOK_SESS + 1, D), jnp.float32)
    total, _ = lax.scan(one_expert, start_total, jnp.arange(EXPERTS, dtype=jnp.int32))
    mixed = total[:, :TOK_SESS]
    feat = (tokens.astype(jnp.float32) + mixed).astype(jnp.bfloat16)
    square = lax.optimization_barrier(jnp.mean(jnp.square(feat.astype(jnp.float32)), axis=-1, keepdims=True))
    normed = (feat.astype(jnp.float32) * lax.rsqrt(square + epsilon) * feat_gain).astype(jnp.bfloat16)
    coarse = jnp.dot(normed.reshape(-1, D), w_proj, preferred_element_type=jnp.float32).astype(jnp.bfloat16)
    coarse = coarse.reshape(SESS, GRID_H, GRID_W, C)
    fine = jnp.repeat(jnp.repeat(coarse, 2, axis=1), 2, axis=2)
    latest = pick_slot(frame_cache, cache_head)
    older = pick_slot(frame_cache, (cache_head + 2) % 3)
    stack = jnp.stack([older, latest, fine])
    framed = jnp.pad(stack, ((0, 0), (0, 0), (1, 1), (1, 1), (0, 0)))
    first = jnp.zeros((SESS * PH * PW, C), jnp.float32)
    for frame_step in range(3):
        for row_step in range(3):
            for col_step in range(3):
                patch = framed[frame_step, :, row_step:row_step + PH, col_step:col_step + PW, :].reshape(-1, C)
                first = first + jnp.dot(patch, conv_time[frame_step, row_step, col_step], preferred_element_type=jnp.float32)
    active = jax.nn.silu(first + bias_time).astype(jnp.bfloat16).reshape(SESS, PH, PW, C)
    bordered = jnp.pad(active, ((0, 0), (1, 1), (1, 1), (0, 0)))
    second = jnp.zeros((SESS * PH * PW, C), jnp.float32)
    for row_step in range(3):
        for col_step in range(3):
            patch = bordered[:, row_step:row_step + PH, col_step:col_step + PW, :].reshape(-1, C)
            second = second + jnp.dot(patch, conv_space[row_step, col_step], preferred_element_type=jnp.float32)
    result = fine.astype(jnp.float32).reshape(-1, C) + second + bias_space
    return result.astype(jnp.bfloat16).reshape(SESS, PH, PW, C)
```

```python
import functools

import jax
import jax.numpy as jnp
from jax import lax
from jax.experimental import pallas as pl
from jax.experimental.pallas import tpu as pltpu
from jax.sharding import PartitionSpec as P

TOPK = 2
GRID_W = 8
HALO = 2
MESH = pl.DeviceIdType.MESH
VMEM = pl.BlockSpec(memory_space=pltpu.VMEM)

epsilon = 1e-06


def partner(me, bits):
    other, weight = me, 1
    while bits:
        if bits & 1:
            other = other + weight * (1 - 2 * ((me // weight) % 2))
        bits //= 2
        weight *= 2
    return other


def exchange_order(count):
    near = min(4, count)
    order = [k for k in range(1, near)]
    for low in range(near):
        for high in range(count // near - 1, 0, -1):
            order.append(high * near + low)
    return order


def enter(me, tile, sessions, tiles):
    barrier = pltpu.get_barrier_semaphore()
    for k in range(1, sessions):
        pl.semaphore_signal(barrier, inc=1, device_id=(partner(me, k), tile), device_id_type=MESH)
    for m in range(1, tiles):
        pl.semaphore_signal(
            barrier, inc=1, device_id=(me, (tile + m) % tiles), device_id_type=MESH
        )
    pl.semaphore_wait(barrier, sessions - 1 + tiles - 1)


def dispatch_kernel(sessions, tiles, cap, src, out, own_sem, send1, recv1, send2, recv2):
    me, tile = lax.axis_index("sess"), lax.axis_index("exp")
    width = src.shape[1]
    part = width // tiles
    columns = pl.ds(pl.multiple_of(tile * part, part), part)

    def rows(index):
        return pl.ds(pl.multiple_of(index * cap, cap), cap)

    enter(me, tile, sessions, tiles)
    own = pltpu.make_async_copy(src.at[rows(me), :], out.at[rows(me), :], own_sem)
    own.start()
    order = exchange_order(sessions)
    copies = {}
    for k in order:
        other = partner(me, k)
        span = slice(None) if k == 1 else columns
        copies[k] = pltpu.make_async_remote_copy(
            src_ref=src.at[rows(other), span],
            dst_ref=out.at[rows(me), span],
            send_sem=send1.at[k],
            recv_sem=recv1.at[k],
            device_id=(other, tile),
            device_id_type=MESH,
        )
        copies[k].start()
    for k in order:
        copies[k].wait_recv()
        if k == 1:
            continue
        block = out.at[rows(partner(me, k)), columns]
        for m in range(1, tiles):
            pltpu.make_async_remote_copy(
                src_ref=block,
                dst_ref=block,
                send_sem=send2.at[m],
                recv_sem=recv2.at[m],
                device_id=(me, (tile + m) % tiles),
                device_id_type=MESH,
            ).start()
    for k in order:
        copies[k].wait_send()
    own.wait()
    passed = out.at[pl.ds(0, (len(order) - 1) * cap), columns]
    for m in range(1, tiles):
        pltpu.make_async_copy(passed, passed, send2.at[m]).wait()
        pltpu.make_async_copy(passed, passed, recv2.at[m]).wait()


def return_kernel(
    sessions,
    tiles,
    cap,
    answer,
    mix_hi,
    mix_lo,
    tokens,
    gain,
    w_proj,
    out,
    stage,
    reduced,
    back,
    mine,
    theirs,
    send_a,
    recv_a,
    send_b,
    recv_b,
    send_c,
    recv_c,
):
    me, tile = lax.axis_index("sess"), lax.axis_index("exp")
    width = answer.shape[1]
    part = width // tiles
    channels = w_proj.shape[1]

    def rows(index):
        return pl.ds(pl.multiple_of(index * cap, cap), cap)

    def columns(index, offset=0, size=part):
        return pl.ds(pl.multiple_of(index * part + offset, 128), size)

    enter(me, tile, sessions, tiles)
    order = exchange_order(sessions)
    order = [k for k in order if k >= 4] + [k for k in order if k < 4] + [0]
    arrivals = {}
    for k in order:
        other = partner(me, k)
        for m in range(1, tiles):
            peer = (tile + m) % tiles
            arrivals[m, k] = pltpu.make_async_remote_copy(
                src_ref=answer.at[rows(other), columns(peer)],
                dst_ref=stage.at[m - 1, rows(other), :],
                send_sem=send_a.at[m],
                recv_sem=recv_a.at[m, k],
                device_id=(me, peer),
                device_id_type=MESH,
            )
            arrivals[m, k].start()
    returns = {}
    for k in order:
        other = partner(me, k)
        total = answer[rows(other), columns(tile)].astype(jnp.float32)
        for m in range(1, tiles):
            arrivals[m, k].wait_recv()
            total = total + stage[m - 1, rows(other), :].astype(jnp.float32)
        if k == 0:
            back[rows(me), :] = total.astype(jnp.bfloat16)
            continue
        reduced[rows(other), :] = total.astype(jnp.bfloat16)
        returns[k] = pltpu.make_async_remote_copy(
            src_ref=reduced.at[rows(other), :],
            dst_ref=back.at[rows(me), :],
            send_sem=send_b.at[k],
            recv_sem=recv_b.at[k],
            device_id=(other, tile),
            device_id_type=MESH,
        )
        returns[k].start()
    for k in order[:-1]:
        returns[k].wait_recv()
    step = min(512, part)
    square = jnp.zeros((tokens.shape[0], 1), jnp.float32)
    coarse = jnp.zeros((tokens.shape[0], channels), jnp.float32)
    for begin in range(0, part, step):
        block = back[:, begin : begin + step]
        mixed = jnp.dot(mix_hi[...], block, preferred_element_type=jnp.float32) + jnp.dot(
            mix_lo[...], block, preferred_element_type=jnp.float32
        )
        span = columns(tile, begin, step)
        feat = (tokens[:, span].astype(jnp.float32) + mixed).astype(jnp.bfloat16)
        feat = feat.astype(jnp.float32)
        square = square + jnp.sum(feat * feat, axis=1, keepdims=True)
        scaled = (feat * gain[:, span]).astype(jnp.bfloat16)
        coarse = coarse + jnp.dot(scaled, w_proj[span, :], preferred_element_type=jnp.float32)
    mine[:, :channels] = coarse
    mine[:, channels:] = jnp.broadcast_to(square, (tokens.shape[0], 128))
    sums = []
    for m in range(1, tiles):
        sums.append(
            pltpu.make_async_remote_copy(
                src_ref=mine,
                dst_ref=theirs.at[m - 1],
                send_sem=send_c.at[m],
                recv_sem=recv_c.at[m],
                device_id=(me, (tile + m) % tiles),
                device_id_type=MESH,
            )
        )
        sums[-1].start()
    for m, copy in enumerate(sums):
        copy.wait_recv()
        coarse = coarse + theirs[m, :, :channels]
        square = square + theirs[m, :, channels : channels + 1]
    out[...] = (coarse * lax.rsqrt(square * (1.0 / width) + epsilon)).astype(jnp.bfloat16)
    for copy in sums:
        copy.wait_send()
    for k in order[:-1]:
        returns[k].wait_send()
    for m in range(1, tiles):
        sent = stage.at[m - 1]
        pltpu.make_async_copy(sent, sent, send_a.at[m]).wait()


def dispatch(outgoing, sessions, tiles, cap):
    return pl.pallas_call(
        functools.partial(dispatch_kernel, sessions, tiles, cap),
        out_shape=jax.ShapeDtypeStruct(outgoing.shape, outgoing.dtype),
        in_specs=[VMEM],
        out_specs=VMEM,
        scratch_shapes=[
            pltpu.SemaphoreType.DMA,
            pltpu.SemaphoreType.DMA((sessions,)),
            pltpu.SemaphoreType.DMA((sessions,)),
            pltpu.SemaphoreType.DMA((tiles,)),
            pltpu.SemaphoreType.DMA((tiles,)),
        ],
        compiler_params=pltpu.CompilerParams(
            collective_id=0, has_side_effects=True, vmem_limit_bytes=30 * 2**20
        ),
        name="dispatch",
    )(outgoing)


def bring_back(answer, mix_hi, mix_lo, tokens, gain, w_proj, sessions, tiles, cap):
    slots, width = answer.shape
    part = width // tiles
    count, channels = tokens.shape[0], w_proj.shape[1]
    return pl.pallas_call(
        functools.partial(return_kernel, sessions, tiles, cap),
        out_shape=jax.ShapeDtypeStruct((count, channels), jnp.bfloat16),
        in_specs=[VMEM] * 6,
        out_specs=VMEM,
        scratch_shapes=[
            pltpu.VMEM((tiles - 1, slots, part), jnp.bfloat16),
            pltpu.VMEM((slots, part), jnp.bfloat16),
            pltpu.VMEM((slots, part), jnp.bfloat16),
            pltpu.VMEM((count, channels + 128), jnp.float32),
            pltpu.VMEM((tiles - 1, count, channels + 128), jnp.float32),
            pltpu.SemaphoreType.DMA((tiles,)),
            pltpu.SemaphoreType.DMA((tiles, sessions)),
            pltpu.SemaphoreType.DMA((sessions,)),
            pltpu.SemaphoreType.DMA((sessions,)),
            pltpu.SemaphoreType.DMA((tiles,)),
            pltpu.SemaphoreType.DMA((tiles,)),
        ],
        compiler_params=pltpu.CompilerParams(
            collective_id=1, has_side_effects=True, vmem_limit_bytes=45 * 2**20
        ),
        name="bring_back",
    )(answer, mix_hi, mix_lo, tokens, gain, w_proj)


def extended(cells, axis, dim, width):
    count = lax.axis_size(axis)
    ends = count - 1
    head = lax.slice_in_dim(cells, 0, width, axis=dim)
    tail = lax.slice_in_dim(cells, cells.shape[dim] - width, cells.shape[dim], axis=dim)
    return jnp.concatenate(
        [
            lax.ppermute(tail, axis, [(i, i + 1) for i in range(ends)]),
            cells,
            lax.ppermute(head, axis, [(i + 1, i) for i in range(ends)]),
        ],
        axis=dim,
    )


def slot_targets(routes, capacity):
    flat = routes.reshape(-1)
    place = jnp.arange(flat.shape[0], dtype=jnp.int32)
    earlier = (flat[:, None] == flat[None, :]) & (place[None, :] < place[:, None])
    return flat * capacity + jnp.sum(earlier.astype(jnp.int32), axis=1)


def patches(frames, height):
    breadth = frames.shape[2]
    padded = jnp.pad(frames, ((0, 0), (0, 0), (1, 1), (0, 0)))
    pieces = [
        padded[t, dy : dy + height, dx : dx + breadth, :]
        for t in range(frames.shape[0])
        for dy in range(3)
        for dx in range(3)
    ]
    return jnp.concatenate(pieces, axis=-1).reshape(height * breadth, -1)


def body(
    tokens,
    routes,
    gates,
    w_gate,
    w_up,
    w_down,
    feat_gain,
    w_proj,
    conv_time,
    bias_time,
    conv_space,
    bias_space,
    frame_cache,
    cache_head,
):
    sessions, tiles = lax.axis_size("sess"), lax.axis_size("exp")
    tile = lax.axis_index("exp")
    channels = w_proj.shape[-1]
    local = tokens[0]
    tok_count = local.shape[0]
    cap = 2 * tok_count * TOPK // sessions
    height, breadth = frame_cache.shape[2:4]
    rows_own = tok_count // tiles

    head = cache_head[0]
    cache = frame_cache[:, 0]
    past = jnp.stack(
        [
            lax.dynamic_index_in_dim(cache, (head + 2) % 3, 0, keepdims=False),
            lax.dynamic_index_in_dim(cache, head, 0, keepdims=False),
        ]
    )
    past = extended(past, "exp", 1, HALO)

    dest = slot_targets(routes[0], cap).reshape(tok_count, TOPK)
    slots = jnp.arange(sessions * cap, dtype=jnp.int32)
    hit = dest[:, :, None] == slots[None, None, :]
    onehot = jnp.any(hit, axis=1).astype(jnp.bfloat16)
    weight = jnp.sum(jnp.where(hit, gates[0][:, :, None], 0.0), axis=1)
    mix_hi = lax.reduce_precision(weight, 8, 7)
    mix_lo = (weight - mix_hi).astype(jnp.bfloat16)
    mix_hi = mix_hi.astype(jnp.bfloat16)
    outgoing = lax.dot_general(
        onehot, local, (((0,), (0,)), ((), ())), preferred_element_type=jnp.float32
    ).astype(jnp.bfloat16)

    rows = dispatch(outgoing, sessions, tiles, cap)
    gate = jnp.dot(rows, w_gate[0], preferred_element_type=jnp.float32)
    upward = jnp.dot(rows, w_up[0], preferred_element_type=jnp.float32)
    hidden = (jax.nn.silu(gate) * upward).astype(jnp.bfloat16)
    answer = jnp.dot(hidden, w_down[0], preferred_element_type=jnp.float32).astype(jnp.bfloat16)
    coarse = bring_back(
        answer, mix_hi, mix_lo, local, feat_gain[None, :], w_proj, sessions, tiles, cap
    )

    coarse = jnp.pad(coarse, ((GRID_W, GRID_W), (0, 0)))
    coarse = lax.dynamic_slice_in_dim(coarse, tile * rows_own, rows_own + 2 * GRID_W, 0)
    coarse = coarse.reshape(-1, GRID_W, channels)
    fine = jnp.repeat(jnp.repeat(coarse, 2, axis=0), 2, axis=1)
    stack = jnp.concatenate([past, fine[None]], axis=0)
    first = jnp.dot(
        patches(stack, height + 2),
        conv_time.reshape(-1, channels),
        preferred_element_type=jnp.float32,
    )
    active = jax.nn.silu(first + bias_time).astype(jnp.bfloat16)
    active = active.reshape(height + 2, breadth, channels)
    row = tile * height - 1 + jnp.arange(height + 2, dtype=jnp.int32)
    inside = (row >= 0) & (row < height * tiles)
    active = jnp.where(inside[:, None, None], active, jnp.zeros_like(active))
    second = jnp.dot(
        patches(active[None], height),
        conv_space.reshape(-1, channels),
        preferred_element_type=jnp.float32,
    )
    own = fine[HALO : HALO + height].reshape(-1, channels)
    result = own.astype(jnp.float32) + second + bias_space
    return result.astype(jnp.bfloat16).reshape(1, height, breadth, channels)


def solution(mesh):
    return jax.shard_map(
        body,
        mesh=mesh,
        in_specs=(
            P("sess", None, None),
            P("sess", None, None),
            P("sess", None, None),
            P("sess", None, "exp"),
            P("sess", None, "exp"),
            P("sess", "exp", None),
            P(),
            P(),
            P(),
            P(),
            P(),
            P(),
            P(None, "sess", "exp", None, None),
            P("sess"),
        ),
        out_specs=P("sess", "exp", None, None),
        check_vma=False,
    )
```

```python
import functools

import jax
import jax.numpy as jnp
from jax import lax
from jax.experimental import pallas as pl
from jax.experimental.pallas import tpu as pltpu
from jax.sharding import PartitionSpec as P

TOPK = 2
GRID_W = 8
HALO = 2
MESH = pl.DeviceIdType.MESH
VMEM = pl.BlockSpec(memory_space=pltpu.VMEM)

epsilon = 1e-06


def partner(me, bits):
    other, weight = me, 1
    while bits:
        if bits & 1:
            other = other + weight * (1 - 2 * ((me // weight) % 2))
        bits //= 2
        weight *= 2
    return other


def exchange_order(count):
    near = min(4, count)
    order = [k for k in range(1, near)]
    for low in range(near):
        for high in range(count // near - 1, 0, -1):
            order.append(high * near + low)
    return order


def enter(me, tile, sessions, tiles):
    barrier = pltpu.get_barrier_semaphore()
    for k in range(1, sessions):
        pl.semaphore_signal(barrier, inc=1, device_id=(partner(me, k), tile), device_id_type=MESH)
    for m in range(1, tiles):
        pl.semaphore_signal(
            barrier, inc=1, device_id=(me, (tile + m) % tiles), device_id_type=MESH
        )
    pl.semaphore_wait(barrier, sessions - 1 + tiles - 1)


def silu(value):
    return value / (1.0 + jnp.exp(-value))


def across(left, right):
    return lax.dot_general(
        left, right, (((1,), (1,)), ((), ())), preferred_element_type=jnp.float32
    )


def dispatch_kernel(
    sessions,
    tiles,
    cap,
    src,
    past,
    w_gate,
    w_up,
    w_down,
    answer,
    halo,
    out,
    gate_w,
    up_w,
    down_w,
    gate,
    upward,
    hidden,
    own_sem,
    load_sem,
    halo_send,
    halo_recv,
    send1,
    recv1,
    send2,
    recv2,
):
    me, tile = lax.axis_index("sess"), lax.axis_index("exp")
    width = src.shape[1]
    part = width // tiles
    columns = pl.ds(pl.multiple_of(tile * part, part), part)

    def rows(index):
        return pl.ds(pl.multiple_of(index * cap, cap), cap)

    loads = [
        pltpu.make_async_copy(source, held, load_sem.at[i])
        for i, (source, held) in enumerate(
            ((w_gate, gate_w), (w_up, up_w), (w_down, down_w))
        )
    ]
    for load in loads:
        load.start()
    enter(me, tile, sessions, tiles)
    own = pltpu.make_async_copy(src.at[rows(me), :], out.at[rows(me), :], own_sem)
    own.start()
    order = exchange_order(sessions)
    copies = {}
    for k in order:
        other = partner(me, k)
        span = slice(None) if k == 1 else columns
        copies[k] = pltpu.make_async_remote_copy(
            src_ref=src.at[rows(other), span],
            dst_ref=out.at[rows(me), span],
            send_sem=send1.at[k],
            recv_sem=recv1.at[k],
            device_id=(other, tile),
            device_id_type=MESH,
        )
        copies[k].start()
    height = past.shape[1]
    borders = []
    for side, begin, step in ((0, height - HALO, 1), (1, 0, tiles - 1)):
        borders.append(
            pltpu.make_async_remote_copy(
                src_ref=past.at[:, begin : begin + HALO],
                dst_ref=halo.at[side],
                send_sem=halo_send.at[side],
                recv_sem=halo_recv.at[side],
                device_id=(me, (tile + step) % tiles),
                device_id_type=MESH,
            )
        )
        borders[-1].start()
    for k in order:
        copies[k].wait_recv()
        if k == 1:
            continue
        block = out.at[rows(partner(me, k)), columns]
        for m in range(1, tiles):
            pltpu.make_async_remote_copy(
                src_ref=block,
                dst_ref=block,
                send_sem=send2.at[m],
                recv_sem=recv2.at[m],
                device_id=(me, (tile + m) % tiles),
                device_id_type=MESH,
            ).start()
    for k in order:
        copies[k].wait_send()
    own.wait()
    passed = out.at[pl.ds(0, (len(order) - 1) * cap), columns]
    for m in range(1, tiles):
        pltpu.make_async_copy(passed, passed, send2.at[m]).wait()
        pltpu.make_async_copy(passed, passed, recv2.at[m]).wait()
    for copy in borders:
        copy.wait()
    for load in loads:
        load.wait()
    depth = width // 4
    gate[...] = jnp.zeros_like(gate)
    upward[...] = jnp.zeros_like(upward)

    @pl.loop(0, width // depth)
    def _(step):
        span = pl.ds(pl.multiple_of(step * depth, depth), depth)
        block = out[:, span]
        gate[...] += across(block, gate_w[:, span])
        upward[...] += across(block, up_w[:, span])

    hidden[...] = (silu(gate[...]) * upward[...]).astype(jnp.bfloat16)
    piece = width // 8

    @pl.loop(0, width // piece)
    def _(step):
        span = pl.ds(pl.multiple_of(step * piece, piece), piece)
        answer[:, span] = jnp.dot(
            hidden[...], down_w[:, span], preferred_element_type=jnp.float32
        ).astype(jnp.bfloat16)


def return_kernel(
    sessions,
    tiles,
    cap,
    answer,
    mix_hi,
    mix_lo,
    all_tokens,
    gain,
    all_proj,
    out,
    tokens,
    w_proj,
    load_sem,
    stage,
    reduced,
    back,
    mine,
    theirs,
    send_a,
    recv_a,
    send_b,
    recv_b,
    send_c,
    recv_c,
):
    me, tile = lax.axis_index("sess"), lax.axis_index("exp")
    width = answer.shape[1]
    part = width // tiles
    channels = w_proj.shape[1]

    def rows(index):
        return pl.ds(pl.multiple_of(index * cap, cap), cap)

    def columns(index, offset=0, size=part):
        return pl.ds(pl.multiple_of(index * part + offset, 128), size)

    loads = [
        pltpu.make_async_copy(all_tokens.at[:, columns(tile)], tokens, load_sem.at[0]),
        pltpu.make_async_copy(all_proj.at[columns(tile), :], w_proj, load_sem.at[1]),
    ]
    for load in loads:
        load.start()
    enter(me, tile, sessions, tiles)
    order = exchange_order(sessions)
    order = [k for k in order if k >= 4] + [k for k in order if k < 4] + [0]
    arrivals = {}
    for k in order:
        other = partner(me, k)
        for m in range(1, tiles):
            peer = (tile + m) % tiles
            arrivals[m, k] = pltpu.make_async_remote_copy(
                src_ref=answer.at[rows(other), columns(peer)],
                dst_ref=stage.at[m - 1, rows(other), :],
                send_sem=send_a.at[m],
                recv_sem=recv_a.at[m, k],
                device_id=(me, peer),
                device_id_type=MESH,
            )
            arrivals[m, k].start()
    returns = {}
    for k in order:
        other = partner(me, k)
        total = answer[rows(other), columns(tile)].astype(jnp.float32)
        for m in range(1, tiles):
            arrivals[m, k].wait_recv()
            total = total + stage[m - 1, rows(other), :].astype(jnp.float32)
        if k == 0:
            back[rows(me), :] = total.astype(jnp.bfloat16)
            continue
        reduced[rows(other), :] = total.astype(jnp.bfloat16)
        returns[k] = pltpu.make_async_remote_copy(
            src_ref=reduced.at[rows(other), :],
            dst_ref=back.at[rows(me), :],
            send_sem=send_b.at[k],
            recv_sem=recv_b.at[k],
            device_id=(other, tile),
            device_id_type=MESH,
        )
        returns[k].start()
    for k in order[:-1]:
        returns[k].wait_recv()
    for load in loads:
        load.wait()
    step = min(512, part)
    square = jnp.zeros((tokens.shape[0], 1), jnp.float32)
    coarse = jnp.zeros((tokens.shape[0], channels), jnp.float32)
    for begin in range(0, part, step):
        block = back[:, begin : begin + step]
        mixed = jnp.dot(mix_hi[...], block, preferred_element_type=jnp.float32) + jnp.dot(
            mix_lo[...], block, preferred_element_type=jnp.float32
        )
        span = columns(tile, begin, step)
        here = slice(begin, begin + step)
        feat = (tokens[:, here].astype(jnp.float32) + mixed).astype(jnp.bfloat16)
        feat = feat.astype(jnp.float32)
        square = square + jnp.sum(feat * feat, axis=1, keepdims=True)
        scaled = (feat * gain[:, span]).astype(jnp.bfloat16)
        coarse = coarse + jnp.dot(scaled, w_proj[here, :], preferred_element_type=jnp.float32)
    mine[:, :channels] = coarse
    mine[:, channels:] = jnp.broadcast_to(square, (tokens.shape[0], 128))
    sums = []
    for m in range(1, tiles):
        sums.append(
            pltpu.make_async_remote_copy(
                src_ref=mine,
                dst_ref=theirs.at[m - 1],
                send_sem=send_c.at[m],
                recv_sem=recv_c.at[m],
                device_id=(me, (tile + m) % tiles),
                device_id_type=MESH,
            )
        )
        sums[-1].start()
    for m, copy in enumerate(sums):
        copy.wait_recv()
        coarse = coarse + theirs[m, :, :channels]
        square = square + theirs[m, :, channels : channels + 1]
    out[...] = (coarse * lax.rsqrt(square * (1.0 / width) + epsilon)).astype(jnp.bfloat16).astype(
        jnp.float32
    )
    for copy in sums:
        copy.wait_send()
    for k in order[:-1]:
        returns[k].wait_send()
    for m in range(1, tiles):
        sent = stage.at[m - 1]
        pltpu.make_async_copy(sent, sent, send_a.at[m]).wait()


def route_kernel(
    sessions, cap, routes, gates, tokens, head, cache, outgoing, mix_hi, mix_lo, past
):
    count = tokens.shape[0]
    slots = sessions * cap
    past[1] = cache[head[0]]
    past[0] = cache[lax.rem(head[0] + 2, 3)]
    expert = lax.broadcasted_iota(jnp.int32, (sessions, count), 0)
    named = [(routes[k : k + 1, :] == expert).astype(jnp.float32) for k in range(TOPK)]
    earlier = lax.broadcasted_iota(jnp.int32, (count, count), 0) < lax.broadcasted_iota(
        jnp.int32, (count, count), 1
    )
    before = jnp.dot(
        sum(named).astype(jnp.bfloat16),
        earlier.astype(jnp.float32).astype(jnp.bfloat16),
        preferred_element_type=jnp.float32,
    )
    slot = lax.broadcasted_iota(jnp.int32, (slots, count), 0)
    onehot = jnp.zeros((slots, count), jnp.float32)
    weight = jnp.zeros((slots, count), jnp.float32)
    for k in range(TOPK):
        place = jnp.sum(before * named[k], axis=0, keepdims=True).astype(jnp.int32)
        hit = slot == routes[k : k + 1, :] * cap + place
        onehot = onehot + jnp.where(hit, 1.0, 0.0)
        weight = weight + jnp.where(hit, gates[k : k + 1, :], 0.0)
        before = before + named[k]
    weight = weight.T
    high = weight.astype(jnp.bfloat16)
    mix_hi[...] = high
    mix_lo[...] = (weight - high.astype(jnp.float32)).astype(jnp.bfloat16)
    onehot = onehot.astype(jnp.bfloat16)
    step = 512
    for begin in range(0, tokens.shape[1], step):
        outgoing[:, begin : begin + step] = jnp.dot(
            onehot, tokens[:, begin : begin + step], preferred_element_type=jnp.float32
        ).astype(jnp.bfloat16)


def route(routes, gates, tokens, head, cache, sessions, cap):
    slots, count = sessions * cap, tokens.shape[0]
    mix = jax.ShapeDtypeStruct((count, slots), jnp.bfloat16)
    return pl.pallas_call(
        functools.partial(route_kernel, sessions, cap),
        out_shape=(
            jax.ShapeDtypeStruct((slots, tokens.shape[1]), jnp.bfloat16),
            mix,
            mix,
            jax.ShapeDtypeStruct((2,) + cache.shape[1:], cache.dtype),
        ),
        in_specs=[VMEM, VMEM, VMEM, pl.BlockSpec(memory_space=pltpu.SMEM), VMEM],
        out_specs=(VMEM,) * 4,
        compiler_params=pltpu.CompilerParams(vmem_limit_bytes=30 * 2**20),
        name="route",
    )(routes, gates, tokens, head, cache)


def conv_kernel(
    coarse,
    past,
    halo,
    w_time,
    bias_time,
    w_space,
    bias_space,
    out,
    above,
    frames,
    wide,
    wide_active,
):
    tile, tiles = lax.axis_index("exp"), lax.axis_size("exp")
    tall, channels = frames.shape[1:]
    breadth = 2 * GRID_W
    edge = HALO * breadth
    count = out.shape[0]
    grid_rows = coarse.shape[0] // GRID_W
    own_rows = grid_rows // tiles

    for r in range(own_rows + 2):
        row = tile * own_rows - 1 + r
        at = jnp.clip(row, 0, grid_rows - 1)
        value = coarse[pl.ds(pl.multiple_of(at * GRID_W, GRID_W), GRID_W), :]
        above[r * GRID_W : (r + 1) * GRID_W, :] = jnp.where(
            (row >= 0) & (row < grid_rows), value, jnp.zeros_like(value)
        )
    for t in range(2):
        top, bottom = halo[0, t], halo[1, t]
        frames[t, :edge, :] = jnp.where(tile > 0, top, jnp.zeros_like(top))
        frames[t, edge : edge + count, :] = past[t]
        frames[t, edge + count :, :] = jnp.where(
            tile < tiles - 1, bottom, jnp.zeros_like(bottom)
        )

    def chosen(mask):
        return jnp.where(mask, 1.0, 0.0).astype(jnp.bfloat16)

    def moved(matrix, value):
        return jnp.dot(matrix, value, preferred_element_type=jnp.float32).astype(jnp.bfloat16)

    few = above.shape[0]
    pixel = lax.broadcasted_iota(jnp.int32, (tall, few), 0)
    token = lax.broadcasted_iota(jnp.int32, (tall, few), 1)
    spread = chosen(token == (pixel // (2 * breadth)) * GRID_W + (pixel % breadth) // 2)
    frames[2] = moved(spread, above[...].astype(jnp.bfloat16))

    def shifts(size):
        to = lax.broadcasted_iota(jnp.int32, (size, size), 0)
        origin = lax.broadcasted_iota(jnp.int32, (size, size), 1)
        column = to % breadth
        return (
            chosen((origin == to - 1) & (column > 0)),
            chosen((origin == to + 1) & (column < breadth - 1)),
        )

    left, right = shifts(tall)
    for t in range(3):
        wide[t, :, :channels] = moved(left, frames[t])
        wide[t, :, channels : 2 * channels] = frames[t]
        wide[t, :, 2 * channels :] = moved(right, frames[t])
    extended = count + 2 * breadth
    first = jnp.zeros((extended, channels), jnp.float32) + bias_time[...]
    for t in range(3):
        for dy in range(3):
            first = first + jnp.dot(
                wide[t, dy * breadth : dy * breadth + extended, :],
                w_time[3 * t + dy],
                preferred_element_type=jnp.float32,
            )
    row = tile * (count // breadth) - 1 + lax.broadcasted_iota(
        jnp.int32, (extended, channels), 0
    ) // breadth
    inside = (row >= 0) & (row < tiles * (count // breadth))
    active = jnp.where(inside, silu(first), 0.0).astype(jnp.bfloat16)
    left, right = shifts(extended)
    wide_active[:, :channels] = moved(left, active)
    wide_active[:, channels : 2 * channels] = active
    wide_active[:, 2 * channels :] = moved(right, active)
    total = frames[2, edge : edge + count, :].astype(jnp.float32) + bias_space[...]
    for dy in range(3):
        total = total + jnp.dot(
            wide_active[dy * breadth : dy * breadth + count, :],
            w_space[dy],
            preferred_element_type=jnp.float32,
        )
    out[...] = total.astype(jnp.bfloat16)


def decode(coarse, past, halo, w_time, bias_time, w_space, bias_space, tiles):
    count, channels = past.shape[1:]
    breadth = 2 * GRID_W
    tall = count + 2 * HALO * breadth
    few = coarse.shape[0] // tiles + 2 * GRID_W
    return pl.pallas_call(
        conv_kernel,
        out_shape=jax.ShapeDtypeStruct((count, channels), jnp.bfloat16),
        in_specs=[VMEM] * 7,
        out_specs=VMEM,
        scratch_shapes=[
            pltpu.VMEM((few, channels), jnp.float32),
            pltpu.VMEM((3, tall, channels), jnp.bfloat16),
            pltpu.VMEM((3, tall, 3 * channels), jnp.bfloat16),
            pltpu.VMEM((count + 2 * breadth, 3 * channels), jnp.bfloat16),
        ],
        compiler_params=pltpu.CompilerParams(vmem_limit_bytes=24 * 2**20),
        name="decode",
    )(coarse, past, halo, w_time, bias_time, w_space, bias_space)


def dispatch(outgoing, past, w_gate, w_up, w_down, sessions, tiles, cap):
    slots, (hid, width) = outgoing.shape[0], w_gate.shape
    hbm = pl.BlockSpec(memory_space=pl.ANY)
    return pl.pallas_call(
        functools.partial(dispatch_kernel, sessions, tiles, cap),
        out_shape=(
            jax.ShapeDtypeStruct(outgoing.shape, outgoing.dtype),
            jax.ShapeDtypeStruct((2, 2, HALO) + past.shape[2:], past.dtype),
        ),
        in_specs=[VMEM, VMEM, hbm, hbm, hbm],
        out_specs=(VMEM, VMEM),
        scratch_shapes=[
            pltpu.VMEM(outgoing.shape, outgoing.dtype),
            pltpu.VMEM((hid, width), jnp.bfloat16),
            pltpu.VMEM((hid, width), jnp.bfloat16),
            pltpu.VMEM((hid, width), jnp.bfloat16),
            pltpu.VMEM((slots, hid), jnp.float32),
            pltpu.VMEM((slots, hid), jnp.float32),
            pltpu.VMEM((slots, hid), jnp.bfloat16),
            pltpu.SemaphoreType.DMA,
            pltpu.SemaphoreType.DMA((3,)),
            pltpu.SemaphoreType.DMA((2,)),
            pltpu.SemaphoreType.DMA((2,)),
            pltpu.SemaphoreType.DMA((sessions,)),
            pltpu.SemaphoreType.DMA((sessions,)),
            pltpu.SemaphoreType.DMA((tiles,)),
            pltpu.SemaphoreType.DMA((tiles,)),
        ],
        compiler_params=pltpu.CompilerParams(
            collective_id=0, has_side_effects=True, vmem_limit_bytes=50 * 2**20
        ),
        name="dispatch",
    )(outgoing, past, w_gate, w_up, w_down)


def bring_back(answer, mix_hi, mix_lo, tokens, gain, w_proj, sessions, tiles, cap):
    slots, width = answer.shape
    part = width // tiles
    count, channels = tokens.shape[0], w_proj.shape[1]
    return pl.pallas_call(
        functools.partial(return_kernel, sessions, tiles, cap),
        out_shape=jax.ShapeDtypeStruct((count, channels), jnp.float32),
        in_specs=[
            VMEM,
            VMEM,
            VMEM,
            pl.BlockSpec(memory_space=pl.ANY),
            VMEM,
            pl.BlockSpec(memory_space=pl.ANY),
        ],
        out_specs=VMEM,
        scratch_shapes=[
            pltpu.VMEM((count, part), jnp.bfloat16),
            pltpu.VMEM((part, channels), jnp.bfloat16),
            pltpu.SemaphoreType.DMA((2,)),
            pltpu.VMEM((tiles - 1, slots, part), jnp.bfloat16),
            pltpu.VMEM((slots, part), jnp.bfloat16),
            pltpu.VMEM((slots, part), jnp.bfloat16),
            pltpu.VMEM((count, channels + 128), jnp.float32),
            pltpu.VMEM((tiles - 1, count, channels + 128), jnp.float32),
            pltpu.SemaphoreType.DMA((tiles,)),
            pltpu.SemaphoreType.DMA((tiles, sessions)),
            pltpu.SemaphoreType.DMA((sessions,)),
            pltpu.SemaphoreType.DMA((sessions,)),
            pltpu.SemaphoreType.DMA((tiles,)),
            pltpu.SemaphoreType.DMA((tiles,)),
        ],
        compiler_params=pltpu.CompilerParams(
            collective_id=1, has_side_effects=True, vmem_limit_bytes=45 * 2**20
        ),
        name="bring_back",
    )(answer, mix_hi, mix_lo, tokens, gain, w_proj)


def body(
    tokens,
    routes,
    gates,
    w_gate,
    w_up,
    w_down,
    feat_gain,
    w_proj,
    conv_time,
    bias_time,
    conv_space,
    bias_space,
    frame_cache,
    cache_head,
):
    sessions, tiles = lax.axis_size("sess"), lax.axis_size("exp")
    channels = w_proj.shape[-1]
    local = tokens[0]
    tok_count = local.shape[0]
    cap = 2 * tok_count * TOPK // sessions
    height, breadth = frame_cache.shape[2:4]
    outgoing, mix_hi, mix_lo, past = route(
        routes[0].T, gates[0].T, local, cache_head, frame_cache[:, 0], sessions, cap
    )
    answer, halo = dispatch(
        outgoing, past, w_gate[0].T, w_up[0].T, w_down[0], sessions, tiles, cap
    )
    coarse = bring_back(
        answer, mix_hi, mix_lo, local, feat_gain[None, :], w_proj, sessions, tiles, cap
    )
    result = decode(
        coarse,
        past.reshape(2, height * breadth, channels),
        halo.reshape(2, 2, HALO * breadth, channels),
        conv_time.reshape(9, 3 * channels, channels),
        bias_time[None, :],
        conv_space.reshape(3, 3 * channels, channels),
        bias_space[None, :],
        tiles,
    )
    return result.reshape(1, height, breadth, channels)


def solution(mesh):
    return jax.shard_map(
        body,
        mesh=mesh,
        in_specs=(
            P("sess", None, None),
            P("sess", None, None),
            P("sess", None, None),
            P("sess", None, "exp"),
            P("sess", None, "exp"),
            P("sess", "exp", None),
            P(),
            P(),
            P(),
            P(),
            P(),
            P(),
            P(None, "sess", "exp", None, None),
            P("sess"),
        ),
        out_specs=P("sess", "exp", None, None),
        check_vma=False,
    )
```

```python
import functools

import jax
import jax.numpy as jnp
from jax import lax
from jax.experimental import pallas as pl
from jax.experimental.pallas import tpu as pltpu
from jax.sharding import PartitionSpec as P

TOPK = 2
GRID_W = 8
HALO = 2
DIRECT = 4
MESH = pl.DeviceIdType.MESH
VMEM = pl.BlockSpec(memory_space=pltpu.VMEM)

epsilon = 1e-06


def partner(me, bits):
    other, weight = me, 1
    while bits:
        if bits & 1:
            other = other + weight * (1 - 2 * ((me // weight) % 2))
        bits //= 2
        weight *= 2
    return other


def exchange_order(count):
    near = min(4, count)
    order = [k for k in range(1, near)]
    for low in range(near):
        for high in range(count // near - 1, 0, -1):
            order.append(high * near + low)
    return order


def enter(me, tile, sessions, tiles):
    barrier = pltpu.get_barrier_semaphore()
    for k in range(1, sessions):
        pl.semaphore_signal(barrier, inc=1, device_id=(partner(me, k), tile), device_id_type=MESH)
    for m in range(1, tiles):
        pl.semaphore_signal(
            barrier, inc=1, device_id=(me, (tile + m) % tiles), device_id_type=MESH
        )
    pl.semaphore_wait(barrier, sessions - 1 + tiles - 1)


def silu(value):
    return value / (1.0 + jnp.exp(-value))


def across(left, right):
    return lax.dot_general(
        left, right, (((1,), (1,)), ((), ())), preferred_element_type=jnp.float32
    )


def dispatch_kernel(
    sessions,
    tiles,
    cap,
    src,
    past,
    w_gate,
    w_up,
    w_down,
    answer,
    halo,
    out,
    gate_w,
    up_w,
    down_w,
    gate,
    upward,
    hidden,
    own_sem,
    load_sem,
    halo_send,
    halo_recv,
    send1,
    recv1,
    send2,
    recv2,
):
    me, tile = lax.axis_index("sess"), lax.axis_index("exp")
    width = src.shape[1]
    part = width // tiles
    columns = pl.ds(pl.multiple_of(tile * part, part), part)

    def rows(index):
        return pl.ds(pl.multiple_of(index * cap, cap), cap)

    loads = [
        pltpu.make_async_copy(source, held, load_sem.at[i])
        for i, (source, held) in enumerate(
            ((w_gate, gate_w), (w_up, up_w), (w_down, down_w))
        )
    ]
    for load in loads:
        load.start()
    enter(me, tile, sessions, tiles)
    own = pltpu.make_async_copy(src.at[rows(me), :], out.at[rows(me), :], own_sem)
    own.start()
    order = exchange_order(sessions)
    copies = {}
    for k in order:
        other = partner(me, k)
        span = slice(None) if k < DIRECT else columns
        copies[k] = pltpu.make_async_remote_copy(
            src_ref=src.at[rows(other), span],
            dst_ref=out.at[rows(me), span],
            send_sem=send1.at[k],
            recv_sem=recv1.at[k],
            device_id=(other, tile),
            device_id_type=MESH,
        )
        copies[k].start()
    height = past.shape[1]
    borders = []
    for side, begin, step in ((0, height - HALO, 1), (1, 0, tiles - 1)):
        borders.append(
            pltpu.make_async_remote_copy(
                src_ref=past.at[:, begin : begin + HALO],
                dst_ref=halo.at[side],
                send_sem=halo_send.at[side],
                recv_sem=halo_recv.at[side],
                device_id=(me, (tile + step) % tiles),
                device_id_type=MESH,
            )
        )
        borders[-1].start()
    for k in order:
        copies[k].wait_recv()
        if k < DIRECT:
            continue
        block = out.at[rows(partner(me, k)), columns]
        for m in range(1, tiles):
            pltpu.make_async_remote_copy(
                src_ref=block,
                dst_ref=block,
                send_sem=send2.at[m],
                recv_sem=recv2.at[m],
                device_id=(me, (tile + m) % tiles),
                device_id_type=MESH,
            ).start()
    for k in order:
        copies[k].wait_send()
    own.wait()
    passed = out.at[pl.ds(0, (sessions - DIRECT) * cap), columns]
    for m in range(1, tiles):
        pltpu.make_async_copy(passed, passed, send2.at[m]).wait()
        pltpu.make_async_copy(passed, passed, recv2.at[m]).wait()
    for copy in borders:
        copy.wait()
    for load in loads:
        load.wait()
    depth = width // 4
    gate[...] = jnp.zeros_like(gate)
    upward[...] = jnp.zeros_like(upward)

    @pl.loop(0, width // depth)
    def _(step):
        span = pl.ds(pl.multiple_of(step * depth, depth), depth)
        block = out[:, span]
        gate[...] += across(block, gate_w[:, span])
        upward[...] += across(block, up_w[:, span])

    hidden[...] = (silu(gate[...]) * upward[...]).astype(jnp.bfloat16)
    piece = width // 8

    @pl.loop(0, width // piece)
    def _(step):
        span = pl.ds(pl.multiple_of(step * piece, piece), piece)
        answer[:, span] = jnp.dot(
            hidden[...], down_w[:, span], preferred_element_type=jnp.float32
        ).astype(jnp.bfloat16)


def return_kernel(
    sessions,
    tiles,
    cap,
    answer,
    mix_hi,
    mix_lo,
    all_tokens,
    gain,
    all_proj,
    out,
    tokens,
    w_proj,
    load_sem,
    stage,
    reduced,
    back,
    mine,
    theirs,
    send_a,
    recv_a,
    send_b,
    recv_b,
    send_c,
    recv_c,
):
    me, tile = lax.axis_index("sess"), lax.axis_index("exp")
    width = answer.shape[1]
    part = width // tiles
    channels = w_proj.shape[1]

    def rows(index):
        return pl.ds(pl.multiple_of(index * cap, cap), cap)

    def columns(index, offset=0, size=part):
        return pl.ds(pl.multiple_of(index * part + offset, 128), size)

    loads = [
        pltpu.make_async_copy(all_tokens.at[:, columns(tile)], tokens, load_sem.at[0]),
        pltpu.make_async_copy(all_proj.at[columns(tile), :], w_proj, load_sem.at[1]),
    ]
    for load in loads:
        load.start()
    enter(me, tile, sessions, tiles)
    order = exchange_order(sessions)
    order = [k for k in order if k >= 4] + [k for k in order if k < 4] + [0]
    arrivals = {}
    for k in order:
        other = partner(me, k)
        for m in range(1, tiles):
            peer = (tile + m) % tiles
            arrivals[m, k] = pltpu.make_async_remote_copy(
                src_ref=answer.at[rows(other), columns(peer)],
                dst_ref=stage.at[m - 1, rows(other), :],
                send_sem=send_a.at[m],
                recv_sem=recv_a.at[m, k],
                device_id=(me, peer),
                device_id_type=MESH,
            )
            arrivals[m, k].start()
    returns = {}
    for k in order:
        other = partner(me, k)
        total = answer[rows(other), columns(tile)].astype(jnp.float32)
        for m in range(1, tiles):
            arrivals[m, k].wait_recv()
            total = total + stage[m - 1, rows(other), :].astype(jnp.float32)
        if k == 0:
            back[rows(me), :] = total.astype(jnp.bfloat16)
            continue
        reduced[rows(other), :] = total.astype(jnp.bfloat16)
        returns[k] = pltpu.make_async_remote_copy(
            src_ref=reduced.at[rows(other), :],
            dst_ref=back.at[rows(me), :],
            send_sem=send_b.at[k],
            recv_sem=recv_b.at[k],
            device_id=(other, tile),
            device_id_type=MESH,
        )
        returns[k].start()
    for k in order[:-1]:
        returns[k].wait_recv()
    for load in loads:
        load.wait()
    step = min(512, part)
    square = jnp.zeros((tokens.shape[0], 1), jnp.float32)
    coarse = jnp.zeros((tokens.shape[0], channels), jnp.float32)
    for begin in range(0, part, step):
        block = back[:, begin : begin + step]
        mixed = jnp.dot(mix_hi[...], block, preferred_element_type=jnp.float32) + jnp.dot(
            mix_lo[...], block, preferred_element_type=jnp.float32
        )
        span = columns(tile, begin, step)
        here = slice(begin, begin + step)
        feat = (tokens[:, here].astype(jnp.float32) + mixed).astype(jnp.bfloat16)
        feat = feat.astype(jnp.float32)
        square = square + jnp.sum(feat * feat, axis=1, keepdims=True)
        scaled = (feat * gain[:, span]).astype(jnp.bfloat16)
        coarse = coarse + jnp.dot(scaled, w_proj[here, :], preferred_element_type=jnp.float32)
    mine[:, :channels] = coarse
    mine[:, channels:] = jnp.broadcast_to(square, (tokens.shape[0], 128))
    sums = []
    for m in range(1, tiles):
        sums.append(
            pltpu.make_async_remote_copy(
                src_ref=mine,
                dst_ref=theirs.at[m - 1],
                send_sem=send_c.at[m],
                recv_sem=recv_c.at[m],
                device_id=(me, (tile + m) % tiles),
                device_id_type=MESH,
            )
        )
        sums[-1].start()
    for m, copy in enumerate(sums):
        copy.wait_recv()
        coarse = coarse + theirs[m, :, :channels]
        square = square + theirs[m, :, channels : channels + 1]
    out[...] = (coarse * lax.rsqrt(square * (1.0 / width) + epsilon)).astype(jnp.bfloat16).astype(
        jnp.float32
    )
    for copy in sums:
        copy.wait_send()
    for k in order[:-1]:
        returns[k].wait_send()
    for m in range(1, tiles):
        sent = stage.at[m - 1]
        pltpu.make_async_copy(sent, sent, send_a.at[m]).wait()


def route_kernel(
    sessions,
    cap,
    all_routes,
    all_gates,
    all_tokens,
    head,
    cache,
    outgoing,
    mix_hi,
    mix_lo,
    past,
    routes,
    gates,
    tokens,
    sems,
):
    count = tokens.shape[0]
    slots = sessions * cap
    loads = [
        pltpu.make_async_copy(source, held, sems.at[i])
        for i, (source, held) in enumerate(
            (
                (all_routes, routes),
                (all_gates, gates),
                (all_tokens, tokens),
                (cache.at[head[0]], past.at[1]),
                (cache.at[lax.rem(head[0] + 2, 3)], past.at[0]),
            )
        )
    ]
    for load in loads:
        load.start()
    for load in loads:
        load.wait()
    expert = lax.broadcasted_iota(jnp.int32, (sessions, count), 0)
    named = [(routes[k : k + 1, :] == expert).astype(jnp.float32) for k in range(TOPK)]
    earlier = lax.broadcasted_iota(jnp.int32, (count, count), 0) < lax.broadcasted_iota(
        jnp.int32, (count, count), 1
    )
    before = jnp.dot(
        sum(named).astype(jnp.bfloat16),
        earlier.astype(jnp.float32).astype(jnp.bfloat16),
        preferred_element_type=jnp.float32,
    )
    slot = lax.broadcasted_iota(jnp.int32, (slots, count), 0)
    onehot = jnp.zeros((slots, count), jnp.float32)
    weight = jnp.zeros((slots, count), jnp.float32)
    for k in range(TOPK):
        place = jnp.sum(before * named[k], axis=0, keepdims=True).astype(jnp.int32)
        hit = slot == routes[k : k + 1, :] * cap + place
        onehot = onehot + jnp.where(hit, 1.0, 0.0)
        weight = weight + jnp.where(hit, gates[k : k + 1, :], 0.0)
        before = before + named[k]
    weight = weight.T
    high = weight.astype(jnp.bfloat16)
    mix_hi[...] = high
    mix_lo[...] = (weight - high.astype(jnp.float32)).astype(jnp.bfloat16)
    onehot = onehot.astype(jnp.bfloat16)
    step = 512
    for begin in range(0, tokens.shape[1], step):
        outgoing[:, begin : begin + step] = jnp.dot(
            onehot, tokens[:, begin : begin + step], preferred_element_type=jnp.float32
        ).astype(jnp.bfloat16)


def route(routes, gates, tokens, head, cache, sessions, cap):
    slots, count = sessions * cap, tokens.shape[0]
    mix = jax.ShapeDtypeStruct((count, slots), jnp.bfloat16)
    hbm = pl.BlockSpec(memory_space=pltpu.HBM)
    return pl.pallas_call(
        functools.partial(route_kernel, sessions, cap),
        out_shape=(
            jax.ShapeDtypeStruct((slots, tokens.shape[1]), jnp.bfloat16),
            mix,
            mix,
            jax.ShapeDtypeStruct((2,) + cache.shape[1:], cache.dtype),
        ),
        in_specs=[hbm, hbm, hbm, pl.BlockSpec(memory_space=pltpu.SMEM), hbm],
        out_specs=(VMEM,) * 4,
        scratch_shapes=[
            pltpu.VMEM(routes.shape, routes.dtype),
            pltpu.VMEM(gates.shape, gates.dtype),
            pltpu.VMEM(tokens.shape, tokens.dtype),
            pltpu.SemaphoreType.DMA((5,)),
        ],
        compiler_params=pltpu.CompilerParams(vmem_limit_bytes=56 * 2**20),
        name="route",
    )(routes, gates, tokens, head, cache)


def conv_kernel(
    coarse,
    past,
    halo,
    w_time,
    bias_time,
    w_space,
    bias_space,
    out,
    above,
    frames,
    wide,
    wide_active,
):
    tile, tiles = lax.axis_index("exp"), lax.axis_size("exp")
    tall, channels = frames.shape[1:]
    breadth = 2 * GRID_W
    edge = HALO * breadth
    count = out.shape[0]
    grid_rows = coarse.shape[0] // GRID_W
    own_rows = grid_rows // tiles

    for r in range(own_rows + 2):
        row = tile * own_rows - 1 + r
        at = jnp.clip(row, 0, grid_rows - 1)
        value = coarse[pl.ds(pl.multiple_of(at * GRID_W, GRID_W), GRID_W), :]
        above[r * GRID_W : (r + 1) * GRID_W, :] = jnp.where(
            (row >= 0) & (row < grid_rows), value, jnp.zeros_like(value)
        )
    for t in range(2):
        top, bottom = halo[0, t], halo[1, t]
        frames[t, :edge, :] = jnp.where(tile > 0, top, jnp.zeros_like(top))
        frames[t, edge : edge + count, :] = past[t]
        frames[t, edge + count :, :] = jnp.where(
            tile < tiles - 1, bottom, jnp.zeros_like(bottom)
        )

    def chosen(mask):
        return jnp.where(mask, 1.0, 0.0).astype(jnp.bfloat16)

    def moved(matrix, value):
        return jnp.dot(matrix, value, preferred_element_type=jnp.float32).astype(jnp.bfloat16)

    few = above.shape[0]
    pixel = lax.broadcasted_iota(jnp.int32, (tall, few), 0)
    token = lax.broadcasted_iota(jnp.int32, (tall, few), 1)
    spread = chosen(token == (pixel // (2 * breadth)) * GRID_W + (pixel % breadth) // 2)
    frames[2] = moved(spread, above[...].astype(jnp.bfloat16))

    def shifts(size):
        to = lax.broadcasted_iota(jnp.int32, (size, size), 0)
        origin = lax.broadcasted_iota(jnp.int32, (size, size), 1)
        column = to % breadth
        return (
            chosen((origin == to - 1) & (column > 0)),
            chosen((origin == to + 1) & (column < breadth - 1)),
        )

    left, right = shifts(tall)
    for t in range(3):
        wide[t, :, :channels] = moved(left, frames[t])
        wide[t, :, channels : 2 * channels] = frames[t]
        wide[t, :, 2 * channels :] = moved(right, frames[t])
    extended = count + 2 * breadth
    first = jnp.zeros((extended, channels), jnp.float32) + bias_time[...]
    for t in range(3):
        for dy in range(3):
            first = first + jnp.dot(
                wide[t, dy * breadth : dy * breadth + extended, :],
                w_time[3 * t + dy],
                preferred_element_type=jnp.float32,
            )
    row = tile * (count // breadth) - 1 + lax.broadcasted_iota(
        jnp.int32, (extended, channels), 0
    ) // breadth
    inside = (row >= 0) & (row < tiles * (count // breadth))
    active = jnp.where(inside, silu(first), 0.0).astype(jnp.bfloat16)
    left, right = shifts(extended)
    wide_active[:, :channels] = moved(left, active)
    wide_active[:, channels : 2 * channels] = active
    wide_active[:, 2 * channels :] = moved(right, active)
    total = frames[2, edge : edge + count, :].astype(jnp.float32) + bias_space[...]
    for dy in range(3):
        total = total + jnp.dot(
            wide_active[dy * breadth : dy * breadth + count, :],
            w_space[dy],
            preferred_element_type=jnp.float32,
        )
    out[...] = total.astype(jnp.bfloat16)


def decode(coarse, past, halo, w_time, bias_time, w_space, bias_space, tiles):
    count, channels = past.shape[1:]
    breadth = 2 * GRID_W
    tall = count + 2 * HALO * breadth
    few = coarse.shape[0] // tiles + 2 * GRID_W
    return pl.pallas_call(
        conv_kernel,
        out_shape=jax.ShapeDtypeStruct((count, channels), jnp.bfloat16),
        in_specs=[VMEM] * 7,
        out_specs=VMEM,
        scratch_shapes=[
            pltpu.VMEM((few, channels), jnp.float32),
            pltpu.VMEM((3, tall, channels), jnp.bfloat16),
            pltpu.VMEM((3, tall, 3 * channels), jnp.bfloat16),
            pltpu.VMEM((count + 2 * breadth, 3 * channels), jnp.bfloat16),
        ],
        compiler_params=pltpu.CompilerParams(vmem_limit_bytes=24 * 2**20),
        name="decode",
    )(coarse, past, halo, w_time, bias_time, w_space, bias_space)


def dispatch(outgoing, past, w_gate, w_up, w_down, sessions, tiles, cap):
    slots, (hid, width) = outgoing.shape[0], w_gate.shape
    hbm = pl.BlockSpec(memory_space=pl.ANY)
    return pl.pallas_call(
        functools.partial(dispatch_kernel, sessions, tiles, cap),
        out_shape=(
            jax.ShapeDtypeStruct(outgoing.shape, outgoing.dtype),
            jax.ShapeDtypeStruct((2, 2, HALO) + past.shape[2:], past.dtype),
        ),
        in_specs=[VMEM, VMEM, hbm, hbm, hbm],
        out_specs=(VMEM, VMEM),
        scratch_shapes=[
            pltpu.VMEM(outgoing.shape, outgoing.dtype),
            pltpu.VMEM((hid, width), jnp.bfloat16),
            pltpu.VMEM((hid, width), jnp.bfloat16),
            pltpu.VMEM((hid, width), jnp.bfloat16),
            pltpu.VMEM((slots, hid), jnp.float32),
            pltpu.VMEM((slots, hid), jnp.float32),
            pltpu.VMEM((slots, hid), jnp.bfloat16),
            pltpu.SemaphoreType.DMA,
            pltpu.SemaphoreType.DMA((3,)),
            pltpu.SemaphoreType.DMA((2,)),
            pltpu.SemaphoreType.DMA((2,)),
            pltpu.SemaphoreType.DMA((sessions,)),
            pltpu.SemaphoreType.DMA((sessions,)),
            pltpu.SemaphoreType.DMA((tiles,)),
            pltpu.SemaphoreType.DMA((tiles,)),
        ],
        compiler_params=pltpu.CompilerParams(
            collective_id=0, has_side_effects=True, vmem_limit_bytes=50 * 2**20
        ),
        name="dispatch",
    )(outgoing, past, w_gate, w_up, w_down)


def bring_back(answer, mix_hi, mix_lo, tokens, gain, w_proj, sessions, tiles, cap):
    slots, width = answer.shape
    part = width // tiles
    count, channels = tokens.shape[0], w_proj.shape[1]
    return pl.pallas_call(
        functools.partial(return_kernel, sessions, tiles, cap),
        out_shape=jax.ShapeDtypeStruct((count, channels), jnp.float32),
        in_specs=[
            VMEM,
            VMEM,
            VMEM,
            pl.BlockSpec(memory_space=pl.ANY),
            VMEM,
            pl.BlockSpec(memory_space=pl.ANY),
        ],
        out_specs=VMEM,
        scratch_shapes=[
            pltpu.VMEM((count, part), jnp.bfloat16),
            pltpu.VMEM((part, channels), jnp.bfloat16),
            pltpu.SemaphoreType.DMA((2,)),
            pltpu.VMEM((tiles - 1, slots, part), jnp.bfloat16),
            pltpu.VMEM((slots, part), jnp.bfloat16),
            pltpu.VMEM((slots, part), jnp.bfloat16),
            pltpu.VMEM((count, channels + 128), jnp.float32),
            pltpu.VMEM((tiles - 1, count, channels + 128), jnp.float32),
            pltpu.SemaphoreType.DMA((tiles,)),
            pltpu.SemaphoreType.DMA((tiles, sessions)),
            pltpu.SemaphoreType.DMA((sessions,)),
            pltpu.SemaphoreType.DMA((sessions,)),
            pltpu.SemaphoreType.DMA((tiles,)),
            pltpu.SemaphoreType.DMA((tiles,)),
        ],
        compiler_params=pltpu.CompilerParams(
            collective_id=1, has_side_effects=True, vmem_limit_bytes=45 * 2**20
        ),
        name="bring_back",
    )(answer, mix_hi, mix_lo, tokens, gain, w_proj)


def body(
    tokens,
    routes,
    gates,
    w_gate,
    w_up,
    w_down,
    feat_gain,
    w_proj,
    conv_time,
    bias_time,
    conv_space,
    bias_space,
    frame_cache,
    cache_head,
):
    sessions, tiles = lax.axis_size("sess"), lax.axis_size("exp")
    channels = w_proj.shape[-1]
    local = tokens[0]
    tok_count = local.shape[0]
    cap = 2 * tok_count * TOPK // sessions
    height, breadth = frame_cache.shape[2:4]
    outgoing, mix_hi, mix_lo, past = route(
        routes[0].T, gates[0].T, local, cache_head, frame_cache[:, 0], sessions, cap
    )
    answer, halo = dispatch(
        outgoing, past, w_gate[0].T, w_up[0].T, w_down[0], sessions, tiles, cap
    )
    coarse = bring_back(
        answer, mix_hi, mix_lo, local, feat_gain[None, :], w_proj, sessions, tiles, cap
    )
    result = decode(
        coarse,
        past.reshape(2, height * breadth, channels),
        halo.reshape(2, 2, HALO * breadth, channels),
        conv_time.reshape(9, 3 * channels, channels),
        bias_time[None, :],
        conv_space.reshape(3, 3 * channels, channels),
        bias_space[None, :],
        tiles,
    )
    return result.reshape(1, height, breadth, channels)


def solution(mesh):
    return jax.shard_map(
        body,
        mesh=mesh,
        in_specs=(
            P("sess", None, None),
            P("sess", None, None),
            P("sess", None, None),
            P("sess", None, "exp"),
            P("sess", None, "exp"),
            P("sess", "exp", None),
            P(),
            P(),
            P(),
            P(),
            P(),
            P(),
            P(None, "sess", "exp", None, None),
            P("sess"),
        ),
        out_specs=P("sess", "exp", None, None),
        check_vma=False,
    )
```
